256 devices in a mesh: dp: 16 (over z, core), seq: 16 (over y, x).
Axes of the slice: x: 4, y: 4, z: 8, core: 2. Of those that a mesh axis runs over, the one named last changes fastest.
Arguments:
- queries: bfloat16 [32768, 64, 128], P(('dp', 'seq')), parts along dimension 0, may hold values from -52 to 52
- keys: bfloat16 [32768, 8, 128], P(('dp', 'seq')), parts along dimension 0, may hold values from -6 to 6
- values: bfloat16 [32768, 8, 128], P(('dp', 'seq')), parts along dimension 0, may hold values from -6 to 6
- doc_ids: int32 [32768], P(('dp', 'seq')), parts along dimension 0, may hold values from 0 to 15, never falling along the last dimension, each value on 1 to 512 neighbouring positions
- counts: int32 [256], P('dp'), parts along dimension 0, may hold values from 64 to 128
Outputs:
- attended: bfloat16 [32768, 64, 128], P(('dp', 'seq')), parts along dimension 0
The draws below stay inside these ranges and needn't reach their ends.
There are 16 independent parts, one for each index of `dp`. The reference program is written for one: setup_inputs(seed, part) draws one part's arguments, and reference() takes and returns one part's arrays. A program takes and returns all parts, laid end to end along the dimension named above; each array names one. Nothing has to cross between parts.
Inputs may be any that keep to these rules, and one draw needn't show every extreme that they name: `doc_ids`: document numbers never fall along the sequence; each document has 1 to 512 positions. The first counts[j] positions of shard j are real tokens, the others padding.
All inputs are finite; a program needn't handle non-finite values.
Results may differ from the reference program's by a relative error of at most 0.003.
Values may be sent and summed in bfloat16 or wider, within the bound.
No kernel may reach another device: no remote copies, remote signals or barrier semaphores. Data moves between devices by JAX's collectives and lax.ppermute only.
A program may use at most 64 MiB of HBM per device.

```python
import math
import jax
import jax.numpy as jnp
import numpy as np
from jax import lax

QUERY_HEAD_COUNT = 64
KEY_VALUE_HEADS = 8
HEAD_WIDTH = 128
S_DEV = 128
BLOCK_POSITIONS = 512
DOC_MOST = 512
SEQUENCE_LENGTH = 2048
DOCS = 16
N_SEQ = 16


def draw_pair(key):
    base = jax.random.fold_in(key, 11)
    key_query, key_random_seed = jax.random.split(base)
    query_draw = jnp.clip(jax.random.normal(key_query, (SEQUENCE_LENGTH, QUERY_HEAD_COUNT, HEAD_WIDTH), jnp.float32), -6.0, 6.0)
    key_sample = jnp.clip(jax.random.normal(key_random_seed, (SEQUENCE_LENGTH, KEY_VALUE_HEADS, HEAD_WIDTH), jnp.float32), -6.0, 6.0)
    return (query_draw, key_sample)


def draw_queries(key, part):
    return draw_pair(key)[0].astype(jnp.bfloat16)


def draw_keys(key, part):
    return draw_pair(key)[1].astype(jnp.bfloat16)


def plant(values, stream_key, low, largest):
    longest = values.shape.index(max(values.shape))
    spots = []
    for shift in (0, 1):
        where = [jax.random.randint(jax.random.fold_in(stream_key, axis), (), 0, length) for axis, length in enumerate(values.shape)]
        where[longest] = (where[longest] + shift) % values.shape[longest]
        spots.append(tuple(where))
    return values.at[spots[0]].set(low).at[spots[1]].set(largest)


def levels(rng, extent, cuts, least, top_value):
    loudness = 1.0
    for dim, blocks in cuts:
        draws = jax.random.uniform(jax.random.fold_in(jax.random.fold_in(rng, 6), dim), (blocks,), jnp.float32, least / len(cuts), top_value / len(cuts))
        loudness = loudness * jnp.repeat(jnp.exp(draws), extent[dim] // blocks).reshape((-1,) + (1,) * (len(extent) - 1 - dim))
    return loudness


def profile(amount, total, most, skew):
    portions = [(1 << 20) // math.isqrt(rank ** skew) + 1 for rank in range(2, amount + 1)]
    surplus, holding = total - most - (amount - 1), [1] * (amount - 1)
    while surplus > 0:
        movable = [i for i in range(amount - 1) if holding[i] < most]
        whole, left = sum([portions[i] for i in movable]), surplus
        for i in movable:
            extra = min(most - holding[i], max(1, left * portions[i] // whole), surplus)
            holding[i] = holding[i] + extra
            surplus = surplus - extra
    return np.array([most] + holding)


def ragged(rng, count, total, most, lean):
    if count == 2:
        one = jax.random.randint(rng, (), max(1, total - most), min(most, total - 1) + 1)
        return jnp.stack([one, total - one])
    lengths = jnp.asarray(profile(count, total, most, lean), jnp.int32)
    twos = (count - 1) // 2
    donor, taker = lengths[1:1 + 2 * twos:2], lengths[2:2 + 2 * twos:2]
    margin = jnp.minimum(donor - 1, most - taker)
    shifted = jax.random.randint(jax.random.fold_in(rng, 1), (twos,), 0, 1 << 20) % (margin + 1)
    lengths = lengths.at[1:1 + 2 * twos:2].set(donor - shifted).at[2:2 + 2 * twos:2].set(taker + shifted)
    return lengths[jax.random.permutation(jax.random.fold_in(rng, 2), count)]


def centred(key, shape, spread, reach, shards=(), held_as=jnp.bfloat16):
    values = spread * jax.random.normal(key, shape, jnp.float32)
    if shards:
        values = values * levels(key, shape, shards, -0.22, 0.18)
    return jnp.clip(values, -reach, reach).astype(held_as)


def setup_inputs(seed: int = 0, part: int = 0) -> dict:
    seeds = jax.random.split(jax.random.key(seed), 6)
    part_keys = jax.random.split(jax.random.fold_in(seeds[5], part), 6)
    return {
        "queries": draw_queries(jax.random.fold_in(jax.random.fold_in(seeds[5], part), 71), part),
        "keys": draw_keys(jax.random.fold_in(jax.random.fold_in(seeds[5], part), 71), part),
        "values": centred(part_keys[2], (SEQUENCE_LENGTH, KEY_VALUE_HEADS, HEAD_WIDTH), 1.0, 6.0, ((0, 16),)),
        "doc_ids": jnp.searchsorted(jnp.cumsum(ragged(part_keys[3], DOCS, SEQUENCE_LENGTH, DOC_MOST, 2)), jnp.arange(SEQUENCE_LENGTH), side="right").astype(jnp.int32),
        "counts": plant(jax.random.randint(part_keys[4], (N_SEQ,), S_DEV // 2, S_DEV + 1), jax.random.fold_in(part_keys[4], 1), S_DEV // 2, S_DEV).astype(jnp.int32),
    }


def reference(queries, keys, values, doc_ids, counts):
    row_count = queries.shape[0]
    shard_rows = row_count // N_SEQ
    queries_per_group = QUERY_HEAD_COUNT // KEY_VALUE_HEADS
    score_scale = 1.0 / math.sqrt(HEAD_WIDTH)
    positions = jnp.arange(row_count, dtype=jnp.int32)
    live_rows = positions % shard_rows < jnp.repeat(counts, shard_rows, total_repeat_length=row_count)
    keys_float = keys.astype(jnp.float32)
    values_float = values.astype(jnp.float32)

    def one_block(start):
        query_tile_rows = lax.dynamic_slice_in_dim(queries, start, BLOCK_POSITIONS, 0).astype(jnp.float32)
        query_tile_rows = query_tile_rows.reshape(BLOCK_POSITIONS, KEY_VALUE_HEADS, queries_per_group, HEAD_WIDTH)
        scores = jnp.einsum('qhgd,khd->hgqk', query_tile_rows, keys_float, precision=lax.Precision.HIGHEST) * score_scale
        query_pos = start + jnp.arange(BLOCK_POSITIONS, dtype=jnp.int32)
        query_doc = lax.dynamic_slice_in_dim(doc_ids, start, BLOCK_POSITIONS, 0)
        query_live = lax.dynamic_slice_in_dim(live_rows, start, BLOCK_POSITIONS, 0)
        allowed = (doc_ids[None, :] == query_doc[:, None]) & (positions[None, :] <= query_pos[:, None]) & live_rows[None, :]
        masked = jnp.where(allowed, scores, -1e+30)
        top = lax.optimization_barrier(jnp.max(masked, axis=-1, keepdims=True))
        weights = jnp.where(allowed, jnp.exp(scores - top), 0.0)
        norm_sum = lax.optimization_barrier(jnp.sum(weights, axis=-1))
        rounded = weights.astype(jnp.bfloat16).astype(jnp.float32)
        mixed = jnp.einsum('hgqk,khd->qhgd', rounded, values_float, precision=lax.Precision.HIGHEST)
        norm_rows = jnp.transpose(norm_sum, (2, 0, 1))[:, :, :, None]
        norm_rows = jnp.where(query_live[:, None, None, None], norm_rows, 1.0)
        output = jnp.where(query_live[:, None, None, None], mixed / norm_rows, 0.0)
        return output.reshape(BLOCK_POSITIONS, QUERY_HEAD_COUNT, HEAD_WIDTH).astype(jnp.bfloat16)
    starts = jnp.arange(0, row_count, BLOCK_POSITIONS, dtype=jnp.int32)
    blocks = lax.map(one_block, starts)
    return blocks.reshape(row_count, QUERY_HEAD_COUNT, HEAD_WIDTH)
```

```python
import functools
import math

import jax
import jax.numpy as jnp
from jax import lax
from jax.experimental import pallas as pl
from jax.experimental.pallas import tpu as pltpu
from jax.sharding import PartitionSpec as P

SPLIT = (4, 4)
ROWS = 512
BACK = (4, 3, 2, 1, 0)
MASKED = -1e30


def attend_kernel(place, counts, q_ref, *refs, scale):
    blocks = len(BACK)
    k_refs, v_refs, d_refs = refs[:blocks], refs[blocks : 2 * blocks], refs[2 * blocks : 3 * blocks]
    out_ref, bias, key_window, value_window = refs[-4:]
    shard, group, width = q_ref.shape
    window = blocks * shard
    me = place[0]

    @pl.when(pl.program_id(0) == 0)
    def _():
        own = d_refs[-1][0:1, :].astype(jnp.float32)
        query_doc = jnp.transpose(jnp.broadcast_to(own, (shard, shard)))
        column = lax.broadcasted_iota(jnp.int32, (shard, shard), 1)
        row = lax.broadcasted_iota(jnp.int32, (shard, shard), 0)
        for i, back in enumerate(BACK):
            live = jnp.where(me >= back, counts[jnp.maximum(me - back, 0)], 0)
            key_doc = jnp.broadcast_to(d_refs[i][0:1, :].astype(jnp.float32), (shard, shard))
            allowed = (key_doc == query_doc) & (column < live)
            if back == 0:
                allowed = allowed & (column <= row)
            here = jnp.where(allowed, 0.0, MASKED)
            bias[:, :, i * shard : (i + 1) * shard] = jnp.broadcast_to(
                here[:, None, :], (shard, group, shard)
            )

    for i in range(blocks):
        key_window[i * shard : (i + 1) * shard, :] = k_refs[i][...]
        value_window[i * shard : (i + 1) * shard, :] = v_refs[i][...]
    count = counts[me]
    tall = ROWS // group
    for start in range(0, shard, tall):
        q = q_ref[start : start + tall].reshape(ROWS, width)
        scores = lax.dot_general(
            q, key_window[...], (((1,), (1,)), ((), ())), preferred_element_type=jnp.float32
        )
        scores = scores + bias[start : start + tall].reshape(ROWS, window)
        top = jnp.max(scores, axis=1, keepdims=True)
        weights = jnp.exp2((scores - top) * scale)
        norm = jnp.sum(weights, axis=1, keepdims=True)
        mixed = jnp.dot(
            weights.astype(jnp.bfloat16), value_window[...], preferred_element_type=jnp.float32
        )
        position = lax.broadcasted_iota(jnp.int32, (ROWS, 1), 0) // group + start
        inverse = jnp.where(position < count, 1.0 / norm, 0.0)
        out_ref[start : start + tall] = (
            (mixed * inverse).astype(jnp.bfloat16).reshape(tall, group, width)
        )


def attend(place, counts, queries, parts, docs, first, heads, kv_heads, earlier):
    shard, query_heads, width = queries.shape
    group = query_heads // kv_heads
    blocks = len(BACK)
    doc_block = [d.shape[0] // 16 - 1 for d in docs]
    window = blocks * shard
    in_specs = [pl.BlockSpec(memory_space=pltpu.SMEM)] * 2
    in_specs += [pl.BlockSpec((shard, group, width), lambda g: (0, first + g, 0))]
    in_specs += [pl.BlockSpec((shard, width), lambda g: (g, 0))] * blocks
    in_specs += [pl.BlockSpec((shard, width), lambda g: (heads + g, 0))] * blocks
    in_specs += [pl.BlockSpec((16, width), lambda g, at=at: (at, 0)) for at in doc_block]
    operands = [place, counts, queries, *parts, *parts, *docs]
    aliases = {}
    if earlier is not None:
        in_specs.append(pl.BlockSpec(memory_space=pl.ANY))
        aliases = {len(operands): 0}
        operands.append(earlier)
    rows = shard * group * heads
    return pl.pallas_call(
        functools.partial(attend_kernel, scale=math.log2(math.e) / math.sqrt(width)),
        grid=(heads,),
        out_shape=jax.ShapeDtypeStruct(queries.shape, jnp.bfloat16),
        in_specs=in_specs,
        out_specs=pl.BlockSpec((shard, group, width), lambda g: (0, first + g, 0)),
        scratch_shapes=[
            pltpu.VMEM((shard, group, window), jnp.float32),
            pltpu.VMEM((window, width), jnp.bfloat16),
            pltpu.VMEM((window, width), jnp.bfloat16),
        ],
        input_output_aliases=aliases,
        compiler_params=pltpu.CompilerParams(vmem_limit_bytes=32 << 20),
        cost_estimate=pl.CostEstimate(
            flops=4 * rows * window * width,
            bytes_accessed=4 * rows * width + 4 * heads * window * width,
            transcendentals=rows * window,
        ),
        name="attend",
    )(*operands)


def row_permute(array, pairs):
    rows = lax.axis_size("seq") // 4
    return lax.ppermute(array, "seq", [(4 * r + i, 4 * r + j) for r in range(rows) for i, j in pairs])


def earlier_shards(own, x):
    size = lax.axis_size("seq")
    back4 = lax.ppermute(own, "seq", [(i, i + 4) for i in range(size - 4)])
    back1 = row_permute(jnp.where(x < 3, own, back4), [(0, 1), (1, 2), (2, 3), (3, 0)])
    back3 = row_permute(jnp.where(x < 1, own, back4), [(0, 3), (1, 0), (2, 1), (3, 2)])
    back2 = row_permute(jnp.where(x % 2 == 0, back1, back3), [(0, 1), (1, 0), (2, 3), (3, 2)])
    return [back4, back3, back2, back1, own]


def local(queries, keys, values, doc_ids, counts):
    shard, kv_heads, width = keys.shape
    device = lax.axis_index("seq")
    x = device % 4
    place = device.reshape(1)
    keys_by_head = jnp.transpose(keys, (1, 0, 2))
    values_by_head = jnp.transpose(values, (1, 0, 2))
    doc_rows = jnp.broadcast_to(doc_ids.astype(jnp.bfloat16)[None], (16, width))
    first = 0
    parts = []
    for i, heads in enumerate(SPLIT):
        pieces = [
            keys_by_head[first : first + heads].reshape(heads * shard, width),
            values_by_head[first : first + heads].reshape(heads * shard, width),
        ]
        if i == 0:
            pieces.append(doc_rows)
        parts.append(earlier_shards(jnp.concatenate(pieces), x))
        first += heads
    result = None
    first = 0
    for i, heads in enumerate(SPLIT):
        result = attend(
            place, counts, queries, parts[i], parts[0], first, heads, kv_heads, result
        )
        first += heads
    return result


def solution(mesh):
    in_specs = (
        P(("dp", "seq"), None, None),
        P(("dp", "seq"), None, None),
        P(("dp", "seq"), None, None),
        P(("dp", "seq")),
        P("dp"),
    )
    out_specs = P(("dp", "seq"), None, None)
    return jax.shard_map(local, mesh=mesh, in_specs=in_specs, out_specs=out_specs, check_vma=False)
```

```python
import functools
import math

import jax
import jax.numpy as jnp
from jax import lax
from jax.experimental import pallas as pl
from jax.experimental.pallas import tpu as pltpu
from jax.sharding import PartitionSpec as P


SPLIT = (2, 3, 3)
ROWS = 512
GROUP = 8
BACK = (4, 3, 2, 1, 0)
MASKED = -1e30


def pack_kernel(docs_hbm, keys_hbm, values_hbm, *refs):
    outs, (docs, keys, values, arrived) = refs[: len(SPLIT)], refs[len(SPLIT) :]
    shard, _, width = keys.shape
    sources = (keys_hbm, values_hbm, docs_hbm)
    copies = [
        pltpu.make_async_copy(source, target, arrived.at[i])
        for i, (source, target) in enumerate(zip(sources, (keys, values, docs)))
    ]
    for copy in copies:
        copy.start()
    for which, ref in ((0, keys), (1, values)):
        copies[which].wait()
        by_head = jnp.swapaxes(ref[...].astype(jnp.float32), 0, 1).astype(jnp.bfloat16)
        first = 0
        for out, heads in zip(outs, SPLIT):
            out[which * heads * shard : (which + 1) * heads * shard, :] = by_head[
                first : first + heads
            ].reshape(heads * shard, width)
            first += heads
    copies[2].wait()
    outs[0][2 * SPLIT[0] * shard :, :] = jnp.broadcast_to(
        docs[...].astype(jnp.float32), (16, width)
    ).astype(jnp.bfloat16)


def pack(doc_ids, keys, values):
    shard, _, width = keys.shape
    rows = [2 * heads * shard + (16 if i == 0 else 0) for i, heads in enumerate(SPLIT)]
    return pl.pallas_call(
        pack_kernel,
        out_shape=[jax.ShapeDtypeStruct((r, width), jnp.bfloat16) for r in rows],
        in_specs=[pl.BlockSpec(memory_space=pltpu.HBM)] * 3,
        out_specs=[pl.BlockSpec(memory_space=pltpu.VMEM)] * len(SPLIT),
        scratch_shapes=[
            pltpu.VMEM((1, width), jnp.int32),
            pltpu.VMEM(keys.shape, keys.dtype),
            pltpu.VMEM(values.shape, values.dtype),
            pltpu.SemaphoreType.DMA((3,)),
        ],
        compiler_params=pltpu.CompilerParams(vmem_limit_bytes=8 << 20),
        name="pack",
    )(
        *[
            pltpu.with_memory_space_constraint(a, pltpu.HBM)
            for a in (doc_ids.reshape(1, width), keys, values)
        ]
    )


def fill_mask(place, counts, docs, mask, shard):
    me = place[0]
    query_doc = jnp.broadcast_to(docs[-1].astype(jnp.float32), (shard, shard))
    query = lax.broadcasted_iota(jnp.int32, (shard, shard), 1)
    key = lax.broadcasted_iota(jnp.int32, (shard, shard), 0)
    for i, back in enumerate(BACK):
        live = jnp.where(me >= back, counts[jnp.maximum(me - back, 0)], 0)
        key_doc = jnp.transpose(jnp.broadcast_to(docs[i].astype(jnp.float32), (shard, shard)))
        allowed = (key_doc == query_doc) & (key < live)
        if back == 0:
            allowed = allowed & (key <= query)
        mask[i * shard : (i + 1) * shard, :] = jnp.where(allowed, 0.0, MASKED).astype(jnp.bfloat16)


def attend_kernel(place, counts, q_ref, *refs, scale, first, heads, makes_mask):
    blocks = len(BACK)
    parts, refs = refs[:blocks], refs[blocks:]
    shard, _, width = q_ref.shape
    group = GROUP
    if makes_mask:
        result, mask, *refs = refs
        at = 2 * heads * shard
        fill_mask(place, counts, [p[at : at + 1, :] for p in parts], mask, shard)
    else:
        mask, _, result, *refs = refs
    select, key_window, value_window, mixed_heads, sent = refs
    position = lax.broadcasted_iota(jnp.int32, (shard * group, shard), 0) // group
    column = lax.broadcasted_iota(jnp.int32, (shard * group, shard), 1)
    select[...] = jnp.where(position == column, 1.0, 0.0).astype(jnp.bfloat16)
    for j in range(heads):
        key_window[j, :, width:] = mask[...]
        for i in range(blocks):
            at = slice(i * shard, (i + 1) * shard)
            key_window[j, at, :width] = parts[i][j * shard : (j + 1) * shard, :]
            value_window[j, at, :] = parts[i][(heads + j) * shard : (heads + j + 1) * shard, :]
    count = counts[place[0]]
    tall = ROWS // group

    def score(j, c):
        at = (first + j) * group
        q = q_ref[c * tall : (c + 1) * tall, at : at + group].reshape(ROWS, width)
        q = jnp.concatenate([q, select[c * ROWS : (c + 1) * ROWS, :]], axis=1)
        return lax.dot_general(
            q, key_window[j], (((1,), (1,)), ((), ())), preferred_element_type=jnp.float32
        )

    def soften(scores):
        top = jnp.max(scores, axis=1, keepdims=True)
        weights = jnp.exp2((scores - top) * scale)
        return weights.astype(jnp.bfloat16), jnp.sum(weights, axis=1, keepdims=True)

    def leave(j):
        at = (first + j) * group
        return pltpu.make_async_copy(
            mixed_heads.at[j], result.at[:, at : at + group, :], sent.at[j]
        )

    def mix(j, c, weights, norm):
        mixed = jnp.dot(weights, value_window[j], preferred_element_type=jnp.float32)
        position = lax.broadcasted_iota(jnp.int32, (ROWS, 1), 0) // group + c * tall
        inverse = jnp.where(position < count, 1.0 / norm, 0.0)
        mixed_heads[j, c * tall : (c + 1) * tall] = (
            (mixed * inverse).astype(jnp.bfloat16).reshape(tall, group, width)
        )
        if (c + 1) * tall == shard:
            leave(j).start()

    work = [(j, c) for j in range(heads) for c in range(shard // tall)]
    scores = score(*work[0])
    waiting = None
    for i, (j, c) in enumerate(work):
        after = score(*work[i + 1]) if i + 1 < len(work) else None
        weights, norm = soften(scores)
        if waiting is not None:
            mix(*waiting)
        waiting = (j, c, weights, norm)
        scores = after
    mix(*waiting)
    for j in range(heads):
        leave(j).wait()


def attend(place, counts, queries, parts, first, heads, before):
    shard, _, width = queries.shape
    window = len(BACK) * shard
    vmem = pl.BlockSpec(memory_space=pltpu.VMEM)
    in_specs = [pl.BlockSpec(memory_space=pltpu.SMEM)] * 2 + [vmem] * (1 + len(BACK))
    operands = [place, counts, queries, *parts]
    out_shape = [jax.ShapeDtypeStruct(queries.shape, jnp.bfloat16)]
    out_specs = [pl.BlockSpec(memory_space=pltpu.HBM)]
    aliases = {}
    if before is None:
        out_shape.append(jax.ShapeDtypeStruct((window, shard), jnp.bfloat16))
        out_specs.append(vmem)
    else:
        result, mask = before
        in_specs += [vmem, pl.BlockSpec(memory_space=pltpu.HBM)]
        aliases = {len(operands) + 1: 0}
        operands += [mask, result]
    rows = shard * GROUP * heads
    out = pl.pallas_call(
        functools.partial(
            attend_kernel,
            scale=math.log2(math.e) / math.sqrt(width),
            first=first,
            heads=heads,
            makes_mask=before is None,
        ),
        out_shape=out_shape,
        in_specs=in_specs,
        out_specs=out_specs,
        scratch_shapes=[
            pltpu.VMEM((shard * GROUP, shard), jnp.bfloat16),
            pltpu.VMEM((heads, window, 2 * width), jnp.bfloat16),
            pltpu.VMEM((heads, window, width), jnp.bfloat16),
            pltpu.VMEM((heads, shard, GROUP, width), jnp.bfloat16),
            pltpu.SemaphoreType.DMA((heads,)),
        ],
        input_output_aliases=aliases,
        compiler_params=pltpu.CompilerParams(vmem_limit_bytes=32 << 20),
        cost_estimate=pl.CostEstimate(
            flops=4 * rows * window * width,
            bytes_accessed=4 * rows * width + 4 * heads * window * width,
            transcendentals=rows * window,
        ),
        name="attend",
    )(*operands)
    return out if before is None else [out[0], mask]


def row_permute(array, pairs):
    rows = lax.axis_size("seq") // 4
    return lax.ppermute(array, "seq", [(4 * r + i, 4 * r + j) for r in range(rows) for i, j in pairs])


def earlier_shards(own, x):
    size = lax.axis_size("seq")
    back4 = lax.ppermute(own, "seq", [(i, i + 4) for i in range(size - 4)])
    back1 = row_permute(jnp.where(x < 3, own, back4), [(0, 1), (1, 2), (2, 3), (3, 0)])
    back3 = row_permute(jnp.where(x < 1, own, back4), [(0, 3), (1, 0), (2, 1), (3, 2)])
    back2 = row_permute(
        jnp.where(x % 2 == 0, back1, back3), [(0, 1), (1, 0), (2, 3), (3, 2)]
    )
    return [back4, back3, back2, back1, own]


def local(queries, keys, values, doc_ids, counts):
    device = lax.axis_index("seq")
    x = device % 4
    place = device.reshape(1)
    parts = []
    for own in pack(doc_ids, keys, values):
        parts.append(earlier_shards(own, x))
    before = None
    first = 0
    for heads, part in zip(SPLIT, parts):
        before = attend(place, counts, queries, part, first, heads, before)
        first += heads
    return before[0]


def solution(mesh):
    in_specs = (
        P(("dp", "seq"), None, None),
        P(("dp", "seq"), None, None),
        P(("dp", "seq"), None, None),
        P(("dp", "seq")),
        P("dp"),
    )
    out_specs = P(("dp", "seq"), None, None)
    return jax.shard_map(local, mesh=mesh, in_specs=in_specs, out_specs=out_specs, check_vma=False)
```

```python
import functools
import math

import jax
import jax.numpy as jnp
from jax import lax
from jax.experimental import pallas as pl
from jax.experimental.pallas import tpu as pltpu
from jax.sharding import PartitionSpec as P


SPLIT = (2, 3, 3)
ROWS = 512
GROUP = 8
BACK = (4, 3, 2, 1, 0)
MASKED = -1e30


def pack_kernel(docs_hbm, keys_hbm, values_hbm, *refs):
    outs, (docs, keys, values, arrived) = refs[: len(SPLIT)], refs[len(SPLIT) :]
    shard, _, width = keys.shape
    sources = (keys_hbm, values_hbm, docs_hbm)
    copies = [
        pltpu.make_async_copy(source, target, arrived.at[i])
        for i, (source, target) in enumerate(zip(sources, (keys, values, docs)))
    ]
    for copy in copies:
        copy.start()
    for which, ref in ((0, keys), (1, values)):
        copies[which].wait()
        by_head = jnp.swapaxes(ref[...].astype(jnp.float32), 0, 1).astype(jnp.bfloat16)
        first = 0
        for out, heads in zip(outs, SPLIT):
            out[which * heads * shard : (which + 1) * heads * shard, :] = by_head[
                first : first + heads
            ].reshape(heads * shard, width)
            first += heads
    copies[2].wait()
    outs[0][2 * SPLIT[0] * shard :, :] = jnp.broadcast_to(
        docs[...].astype(jnp.float32), (16, width)
    ).astype(jnp.bfloat16)


def pack(doc_ids, keys, values):
    shard, _, width = keys.shape
    rows = [2 * heads * shard + (16 if i == 0 else 0) for i, heads in enumerate(SPLIT)]
    return pl.pallas_call(
        pack_kernel,
        out_shape=[jax.ShapeDtypeStruct((r, width), jnp.bfloat16) for r in rows],
        in_specs=[pl.BlockSpec(memory_space=pltpu.HBM)] * 3,
        out_specs=[pl.BlockSpec(memory_space=pltpu.VMEM)] * len(SPLIT),
        scratch_shapes=[
            pltpu.VMEM((1, width), jnp.int32),
            pltpu.VMEM(keys.shape, keys.dtype),
            pltpu.VMEM(values.shape, values.dtype),
            pltpu.SemaphoreType.DMA((3,)),
        ],
        compiler_params=pltpu.CompilerParams(vmem_limit_bytes=8 << 20),
        name="pack",
    )(
        *[
            pltpu.with_memory_space_constraint(a, pltpu.HBM)
            for a in (doc_ids.reshape(1, width), keys, values)
        ]
    )


def fill_mask(place, counts, docs, mask, shard):
    me = place[0]
    query_doc = jnp.broadcast_to(docs[-1].astype(jnp.float32), (shard, shard))
    query = lax.broadcasted_iota(jnp.int32, (shard, shard), 1)
    key = lax.broadcasted_iota(jnp.int32, (shard, shard), 0)
    for i, back in enumerate(BACK):
        live = jnp.where(me >= back, counts[jnp.maximum(me - back, 0)], 0)
        key_doc = jnp.transpose(jnp.broadcast_to(docs[i].astype(jnp.float32), (shard, shard)))
        allowed = (key_doc == query_doc) & (key < live)
        if back == 0:
            allowed = allowed & (key <= query)
        mask[i * shard : (i + 1) * shard, :] = jnp.where(allowed, 0.0, MASKED).astype(jnp.bfloat16)


def attend_kernel(place, counts, q_ref, *refs, scale, starts, heads, makes_mask):
    blocks = len(BACK)
    parts, refs = refs[:blocks], list(refs[blocks:])
    shard, _, width = q_ref.shape
    group = GROUP
    first = starts[-1]
    last = first + heads == sum(SPLIT)
    mask = refs.pop(0) if not makes_mask else None
    others = [refs.pop(0) for _ in starts[:-1]] if last else []
    out_ref = refs.pop(0)
    if makes_mask:
        mask = refs.pop(0)
        at = 2 * heads * shard
        fill_mask(place, counts, [p[at : at + 1, :] for p in parts], mask, shard)
    select, key_window, value_window = refs[:3]
    copies = []

    def send(source, rows, head):
        at = head * group
        copies.append(
            pltpu.make_async_copy(
                source, out_ref.at[rows, at : at + group, :], refs[4].at[len(copies)]
            )
        )
        copies[-1].start()

    for other, start in zip(others, starts):
        for j in range(other.shape[0]):
            send(other.at[j], slice(0, shard), start + j)
    mixed_heads = refs[3] if last else out_ref
    position = lax.broadcasted_iota(jnp.int32, (shard * group, shard), 0) // group
    column = lax.broadcasted_iota(jnp.int32, (shard * group, shard), 1)
    select[...] = jnp.where(position == column, 1.0, 0.0).astype(jnp.bfloat16)
    for j in range(heads):
        key_window[j, :, width:] = mask[...]
        for i in range(blocks):
            at = slice(i * shard, (i + 1) * shard)
            key_window[j, at, :width] = parts[i][j * shard : (j + 1) * shard, :]
            value_window[j, at, :] = parts[i][(heads + j) * shard : (heads + j + 1) * shard, :]
    count = counts[place[0]]
    tall = ROWS // group

    def score(j, c):
        at = (first + j) * group
        q = q_ref[c * tall : (c + 1) * tall, at : at + group].reshape(ROWS, width)
        q = jnp.concatenate([q, select[c * ROWS : (c + 1) * ROWS, :]], axis=1)
        return lax.dot_general(
            q, key_window[j], (((1,), (1,)), ((), ())), preferred_element_type=jnp.float32
        )

    def soften(scores):
        top = jnp.max(scores, axis=1, keepdims=True)
        weights = jnp.exp2((scores - top) * scale)
        return weights.astype(jnp.bfloat16), jnp.sum(weights, axis=1, keepdims=True)

    def mix(j, c, weights, norm):
        mixed = jnp.dot(weights, value_window[j], preferred_element_type=jnp.float32)
        position = lax.broadcasted_iota(jnp.int32, (ROWS, 1), 0) // group + c * tall
        inverse = jnp.where(position < count, 1.0 / norm, 0.0)
        mixed_heads[j, c * tall : (c + 1) * tall] = (
            (mixed * inverse).astype(jnp.bfloat16).reshape(tall, group, width)
        )
        if last:
            rows = slice(c * tall, (c + 1) * tall)
            send(mixed_heads.at[j, rows], rows, first + j)

    work = [(j, c) for j in range(heads) for c in range(shard // tall)]
    scores = score(*work[0])
    waiting = None
    for i, (j, c) in enumerate(work):
        after = score(*work[i + 1]) if i + 1 < len(work) else None
        weights, norm = soften(scores)
        if waiting is not None:
            mix(*waiting)
        waiting = (j, c, weights, norm)
        scores = after
    mix(*waiting)
    for copy in copies:
        copy.wait()


def attend(place, counts, queries, parts, starts, heads, mask, others):
    shard, _, width = queries.shape
    window = len(BACK) * shard
    last = starts[-1] + heads == sum(SPLIT)
    vmem = pl.BlockSpec(memory_space=pltpu.VMEM)
    in_specs = [pl.BlockSpec(memory_space=pltpu.SMEM)] * 2 + [vmem] * (1 + len(BACK))
    operands = [place, counts, queries, *parts]
    mixed = (heads, shard, GROUP, width)
    if last:
        out_shape = [jax.ShapeDtypeStruct(queries.shape, jnp.bfloat16)]
        out_specs = [pl.BlockSpec(memory_space=pltpu.HBM)]
    else:
        out_shape = [jax.ShapeDtypeStruct(mixed, jnp.bfloat16)]
        out_specs = [vmem]
    if mask is None:
        out_shape.append(jax.ShapeDtypeStruct((window, shard), jnp.bfloat16))
        out_specs.append(vmem)
    else:
        operands.append(mask)
        in_specs.append(vmem)
    scratch = [
        pltpu.VMEM((shard * GROUP, shard), jnp.bfloat16),
        pltpu.VMEM((heads, window, 2 * width), jnp.bfloat16),
        pltpu.VMEM((heads, window, width), jnp.bfloat16),
    ]
    if last:
        operands += others
        in_specs += [vmem] * len(others)
        pieces = starts[-1] + heads * (shard * GROUP // ROWS)
        scratch += [pltpu.VMEM(mixed, jnp.bfloat16), pltpu.SemaphoreType.DMA((pieces,))]
    rows = shard * GROUP * heads
    out = pl.pallas_call(
        functools.partial(
            attend_kernel,
            scale=math.log2(math.e) / math.sqrt(width),
            starts=tuple(starts),
            heads=heads,
            makes_mask=mask is None,
        ),
        out_shape=out_shape,
        in_specs=in_specs,
        out_specs=out_specs,
        scratch_shapes=scratch,
        compiler_params=pltpu.CompilerParams(vmem_limit_bytes=32 << 20),
        cost_estimate=pl.CostEstimate(
            flops=4 * rows * window * width,
            bytes_accessed=4 * rows * width + 4 * heads * window * width,
            transcendentals=rows * window,
        ),
        name="attend",
    )(*operands)
    return out[0], out[1] if mask is None else mask


def row_permute(array, pairs):
    rows = lax.axis_size("seq") // 4
    return lax.ppermute(array, "seq", [(4 * r + i, 4 * r + j) for r in range(rows) for i, j in pairs])


def earlier_shards(own, x, direct):
    size = lax.axis_size("seq")
    back4 = lax.ppermute(own, "seq", [(i, (i + 4) % size) for i in range(size)])
    if direct:
        back3 = lax.ppermute(own, "seq", [(i, (i + 3) % size) for i in range(size)])
    else:
        back3 = row_permute(jnp.where(x < 1, own, back4), [(0, 3), (1, 0), (2, 1), (3, 2)])
    if direct:
        back1 = lax.ppermute(own, "seq", [(i, (i + 1) % size) for i in range(size)])
    else:
        back1 = row_permute(jnp.where(x < 3, own, back4), [(0, 1), (1, 2), (2, 3), (3, 0)])
    back2 = row_permute(
        jnp.where(x % 2 == 0, back1, back3), [(0, 1), (1, 0), (2, 3), (3, 2)]
    )
    return [back4, back3, back2, back1, own]


def local(queries, keys, values, doc_ids, counts):
    device = lax.axis_index("seq")
    x = device % 4
    place = device.reshape(1)
    parts = []
    for own in pack(doc_ids, keys, values):
        parts.append(earlier_shards(own, x, False))
    mask = None
    starts, mixed = [], []
    for i, (heads, part) in enumerate(zip(SPLIT, parts)):
        starts.append(sum(SPLIT[:i]))
        out, mask = attend(place, counts, queries, part, starts, heads, mask, mixed)
        mixed.append(out)
    return mixed[-1]


def solution(mesh):
    in_specs = (
        P(("dp", "seq"), None, None),
        P(("dp", "seq"), None, None),
        P(("dp", "seq"), None, None),
        P(("dp", "seq")),
        P("dp"),
    )
    out_specs = P(("dp", "seq"), None, None)
    return jax.shard_map(local, mesh=mesh, in_specs=in_specs, out_specs=out_specs, check_vma=False)
```

```python
import functools
import math

import jax
import jax.numpy as jnp
from jax import lax
from jax.experimental import pallas as pl
from jax.experimental.pallas import tpu as pltpu
from jax.sharding import PartitionSpec as P


SPLIT = (2, 3, 3)
ROWS = 512
GROUP = 8
BACK = (4, 3, 2, 1, 0)
MASKED = -1e30


def pack_kernel(docs_hbm, keys_hbm, values_hbm, *refs):
    outs, (docs, keys, values, arrived) = refs[: len(SPLIT)], refs[len(SPLIT) :]
    shard, _, width = keys.shape
    sources = (keys_hbm, values_hbm, docs_hbm)
    copies = [
        pltpu.make_async_copy(source, target, arrived.at[i])
        for i, (source, target) in enumerate(zip(sources, (keys, values, docs)))
    ]
    for copy in copies:
        copy.start()
    for which, ref in ((0, keys), (1, values)):
        copies[which].wait()
        by_head = jnp.swapaxes(ref[...].astype(jnp.float32), 0, 1).astype(jnp.bfloat16)
        first = 0
        for out, heads in zip(outs, SPLIT):
            out[which * heads * shard : (which + 1) * heads * shard, :] = by_head[
                first : first + heads
            ].reshape(heads * shard, width)
            first += heads
    copies[2].wait()
    outs[0][2 * SPLIT[0] * shard :, :] = jnp.broadcast_to(
        docs[...].astype(jnp.float32), (16, width)
    ).astype(jnp.bfloat16)


def pack(doc_ids, keys, values):
    shard, _, width = keys.shape
    rows = [2 * heads * shard + (16 if i == 0 else 0) for i, heads in enumerate(SPLIT)]
    return pl.pallas_call(
        pack_kernel,
        out_shape=[jax.ShapeDtypeStruct((r, width), jnp.bfloat16) for r in rows],
        in_specs=[pl.BlockSpec(memory_space=pltpu.HBM)] * 3,
        out_specs=[pl.BlockSpec(memory_space=pltpu.VMEM)] * len(SPLIT),
        scratch_shapes=[
            pltpu.VMEM((1, width), jnp.int32),
            pltpu.VMEM(keys.shape, keys.dtype),
            pltpu.VMEM(values.shape, values.dtype),
            pltpu.SemaphoreType.DMA((3,)),
        ],
        compiler_params=pltpu.CompilerParams(vmem_limit_bytes=8 << 20),
        name="pack",
    )(
        *[
            pltpu.with_memory_space_constraint(a, pltpu.HBM)
            for a in (doc_ids.reshape(1, width), keys, values)
        ]
    )


def prepare_kernel(payload, select):
    position = lax.broadcasted_iota(jnp.int32, select.shape, 0) // GROUP
    column = lax.broadcasted_iota(jnp.int32, select.shape, 1)
    select[...] = jnp.where(position == column, 1.0, 0.0).astype(jnp.bfloat16)


def prepare(payload, shard):
    vmem = pl.BlockSpec(memory_space=pltpu.VMEM)
    return pl.pallas_call(
        prepare_kernel,
        out_shape=jax.ShapeDtypeStruct((shard * GROUP, shard), jnp.bfloat16),
        in_specs=[vmem],
        out_specs=vmem,
        compiler_params=pltpu.CompilerParams(vmem_limit_bytes=8 << 20),
        name="prepare",
    )(payload)


def fill_mask(place, counts, docs, mask, shard):
    me = place[0]
    query_doc = jnp.broadcast_to(docs[-1].astype(jnp.float32), (shard, shard))
    query = lax.broadcasted_iota(jnp.int32, (shard, shard), 1)
    key = lax.broadcasted_iota(jnp.int32, (shard, shard), 0)
    for i, back in enumerate(BACK):
        live = jnp.where(me >= back, counts[jnp.maximum(me - back, 0)], 0)
        key_doc = jnp.transpose(jnp.broadcast_to(docs[i].astype(jnp.float32), (shard, shard)))
        allowed = (key_doc == query_doc) & (key < live)
        if back == 0:
            allowed = allowed & (key <= query)
        mask[i * shard : (i + 1) * shard, :] = jnp.where(allowed, 0.0, MASKED).astype(jnp.bfloat16)


def attend_kernel(place, counts, select, q_ref, *refs, scale, starts, heads, makes_mask):
    blocks = len(BACK)
    parts, refs = refs[:blocks], list(refs[blocks:])
    shard, _, width = q_ref.shape
    group = GROUP
    first = starts[-1]
    last = first + heads == sum(SPLIT)
    mask = refs.pop(0) if not makes_mask else None
    others = [refs.pop(0) for _ in starts[:-1]] if last else []
    out_ref = refs.pop(0)
    if makes_mask:
        mask = refs.pop(0)
        at = 2 * heads * shard
        fill_mask(place, counts, [p[at : at + 1, :] for p in parts], mask, shard)
    key_window, value_window = refs[:2]
    copies = []

    def send(source, rows, head):
        at = head * group
        copies.append(
            pltpu.make_async_copy(
                source, out_ref.at[rows, at : at + group, :], refs[3].at[len(copies)]
            )
        )
        copies[-1].start()

    for other, start in zip(others, starts):
        for j in range(other.shape[0]):
            send(other.at[j], slice(0, shard), start + j)
    mixed_heads = refs[2] if last else out_ref
    for j in range(heads):
        key_window[j, :, width:] = mask[...]
        for i in range(blocks):
            at = slice(i * shard, (i + 1) * shard)
            key_window[j, at, :width] = parts[i][j * shard : (j + 1) * shard, :]
            value_window[j, at, :] = parts[i][(heads + j) * shard : (heads + j + 1) * shard, :]
    count = counts[place[0]]
    tall = ROWS // group

    def score(j, c):
        at = (first + j) * group
        q = q_ref[c * tall : (c + 1) * tall, at : at + group].reshape(ROWS, width)
        q = jnp.concatenate([q, select[c * ROWS : (c + 1) * ROWS, :]], axis=1)
        return lax.dot_general(
            q, key_window[j], (((1,), (1,)), ((), ())), preferred_element_type=jnp.float32
        )

    def soften(scores):
        top = jnp.max(scores, axis=1, keepdims=True)
        weights = jnp.exp2((scores - top) * scale)
        return weights.astype(jnp.bfloat16), jnp.sum(weights, axis=1, keepdims=True)

    def mix(j, c, weights, norm):
        mixed = jnp.dot(weights, value_window[j], preferred_element_type=jnp.float32)
        position = lax.broadcasted_iota(jnp.int32, (ROWS, 1), 0) // group + c * tall
        inverse = jnp.where(position < count, 1.0 / norm, 0.0)
        mixed_heads[j, c * tall : (c + 1) * tall] = (
            (mixed * inverse).astype(jnp.bfloat16).reshape(tall, group, width)
        )
        if last:
            rows = slice(c * tall, (c + 1) * tall)
            send(mixed_heads.at[j, rows], rows, first + j)

    work = [(j, c) for j in range(heads) for c in range(shard // tall)]
    scores = score(*work[0])
    waiting = None
    for i, (j, c) in enumerate(work):
        after = score(*work[i + 1]) if i + 1 < len(work) else None
        weights, norm = soften(scores)
        if waiting is not None:
            mix(*waiting)
        waiting = (j, c, weights, norm)
        scores = after
    mix(*waiting)
    for copy in copies:
        copy.wait()


def attend(place, counts, select, queries, parts, starts, heads, mask, others):
    shard, _, width = queries.shape
    window = len(BACK) * shard
    last = starts[-1] + heads == sum(SPLIT)
    vmem = pl.BlockSpec(memory_space=pltpu.VMEM)
    in_specs = [pl.BlockSpec(memory_space=pltpu.SMEM)] * 2 + [vmem] * (2 + len(BACK))
    operands = [place, counts, select, queries, *parts]
    mixed = (heads, shard, GROUP, width)
    if last:
        out_shape = [jax.ShapeDtypeStruct(queries.shape, jnp.bfloat16)]
        out_specs = [pl.BlockSpec(memory_space=pltpu.HBM)]
    else:
        out_shape = [jax.ShapeDtypeStruct(mixed, jnp.bfloat16)]
        out_specs = [vmem]
    if mask is None:
        out_shape.append(jax.ShapeDtypeStruct((window, shard), jnp.bfloat16))
        out_specs.append(vmem)
    else:
        operands.append(mask)
        in_specs.append(vmem)
    scratch = [
        pltpu.VMEM((heads, window, 2 * width), jnp.bfloat16),
        pltpu.VMEM((heads, window, width), jnp.bfloat16),
    ]
    if last:
        operands += others
        in_specs += [vmem] * len(others)
        pieces = starts[-1] + heads * (shard * GROUP // ROWS)
        scratch += [pltpu.VMEM(mixed, jnp.bfloat16), pltpu.SemaphoreType.DMA((pieces,))]
    rows = shard * GROUP * heads
    out = pl.pallas_call(
        functools.partial(
            attend_kernel,
            scale=math.log2(math.e) / math.sqrt(width),
            starts=tuple(starts),
            heads=heads,
            makes_mask=mask is None,
        ),
        out_shape=out_shape,
        in_specs=in_specs,
        out_specs=out_specs,
        scratch_shapes=scratch,
        compiler_params=pltpu.CompilerParams(vmem_limit_bytes=32 << 20),
        cost_estimate=pl.CostEstimate(
            flops=4 * rows * window * width,
            bytes_accessed=4 * rows * width + 4 * heads * window * width,
            transcendentals=rows * window,
        ),
        name="attend",
    )(*operands)
    return out[0], out[1] if mask is None else mask


def row_permute(array, pairs):
    rows = lax.axis_size("seq") // 4
    return lax.ppermute(array, "seq", [(4 * r + i, 4 * r + j) for r in range(rows) for i, j in pairs])


def earlier_shards(own, x, direct):
    size = lax.axis_size("seq")
    back4 = lax.ppermute(own, "seq", [(i, (i + 4) % size) for i in range(size)])
    if direct:
        back3 = lax.ppermute(own, "seq", [(i, (i + 3) % size) for i in range(size)])
    else:
        back3 = row_permute(jnp.where(x < 1, own, back4), [(0, 3), (1, 0), (2, 1), (3, 2)])
    if direct:
        back1 = lax.ppermute(own, "seq", [(i, (i + 1) % size) for i in range(size)])
    else:
        back1 = row_permute(jnp.where(x < 3, own, back4), [(0, 1), (1, 2), (2, 3), (3, 0)])
    back2 = row_permute(
        jnp.where(x % 2 == 0, back1, back3), [(0, 1), (1, 0), (2, 3), (3, 2)]
    )
    return [back4, back3, back2, back1, own]


def local(queries, keys, values, doc_ids, counts):
    device = lax.axis_index("seq")
    x = device % 4
    place = device.reshape(1)
    parts = []
    for own in pack(doc_ids, keys, values):
        parts.append(earlier_shards(own, x, False))
    select = prepare(parts[0][-1], queries.shape[0])
    mask = None
    starts, mixed = [], []
    for i, (heads, part) in enumerate(zip(SPLIT, parts)):
        starts.append(sum(SPLIT[:i]))
        out, mask = attend(place, counts, select, queries, part, starts, heads, mask, mixed)
        mixed.append(out)
    return mixed[-1]


def solution(mesh):
    in_specs = (
        P(("dp", "seq"), None, None),
        P(("dp", "seq"), None, None),
        P(("dp", "seq"), None, None),
        P(("dp", "seq")),
        P("dp"),
    )
    out_specs = P(("dp", "seq"), None, None)
    return jax.shard_map(local, mesh=mesh, in_specs=in_specs, out_specs=out_specs, check_vma=False)
```
